32 devices in a mesh: ctx: 8 (over z, y), grp: 4 (over x, core).
Axes of the slice: x: 2, y: 2, z: 4, core: 2. Of those that a mesh axis runs over, the one named last changes fastest.
Arguments:
- q_latent: bfloat16 [2048, 1536], P('ctx'), may hold values from -210 to 210
- kv_latent: bfloat16 [2048, 576], P('ctx'), may hold values from -6 to 6
- kv_gain: float32 [512], replicated, may hold values from 0.1 to 1.9
- q_weight: bfloat16 [1536, 6144], P('ctx', 'grp'), may hold values from -0.15625 to 0.15625
- kv_weight: bfloat16 [512, 8192], P('ctx', 'grp'), may hold values from -0.25 to 0.25
- out_weight: bfloat16 [4096, 7168], P('grp', 'ctx'), may hold values from -0.125 to 0.125
- documents: int32 [2048], replicated, may hold values from 0 to 3, never falling along the last dimension, each value on 1 to 1024 neighbouring positions
Outputs:
- mixed: bfloat16 [2048, 7168], P('ctx', 'grp')
The draws below stay inside these ranges and needn't reach their ends.
All inputs are finite; a program needn't handle non-finite values.
Results may differ from the reference program's by a relative error of at most 0.018.
Values may be sent and summed in bfloat16 or wider, within the bound.
No kernel may reach another device: no remote copies, remote signals or barrier semaphores. Data moves between devices by JAX's collectives and lax.ppermute only.
A program may use at most 64 MiB of HBM per device.

```python
import math
import jax
import jax.numpy as jnp
import numpy as np
from jax import lax

D = 7168
QL = 1536
KL = 512
NOPE = 128
ROPE = 64
VDIM = 128
HEAD_DEV = 8
TOK_DEV = 256
HEADS = 32
TOKENS = 2048
N_CTX = 8
N_GRP = 4


def draw_q_latent(key, part):
    sample = jnp.clip(jax.random.normal(key, (TOKENS, QL), jnp.float32), -6.0, 6.0)
    return sample.astype(jnp.bfloat16)


def with_spikes(values, own_key, source, target, blocks, factor):
    owner, partner = [(jnp.arange(values.shape[axis_at]) // (values.shape[axis_at] // blocks)).reshape([-1 if axis == axis_at else 1 for axis in range(values.ndim)]) for axis_at in (source, target)]
    chosen = jax.random.permutation(own_key, blocks)[partner]
    strong = (owner == chosen) | (owner == (partner + blocks // 2) % blocks)
    return jnp.where(strong, factor * values, values)


def level_of(stream_key, extent, pieces, low, top_value):
    def one(position, blocks):
        heights = jax.random.uniform(jax.random.fold_in(jax.random.fold_in(stream_key, 6), position), (blocks,), jnp.float32, low / len(pieces), top_value / len(pieces))
        return jnp.repeat(jnp.exp(heights), extent[position] // blocks).reshape((-1,) + (1,) * (len(extent) - position - 1))

    factor_of = one(*pieces[0])
    for cut in pieces[1:]:
        factor_of = factor_of * one(*cut)
    return factor_of


def split_up(number_of, total, most, skew):
    portions = [(1 << 20) // math.isqrt(grade ** skew) + 1 for grade in range(2, number_of + 1)]
    surplus, given = total - most - (number_of - 1), [1] * (number_of - 1)
    while surplus > 0:
        candidates = [i for i in range(number_of - 1) if given[i] < most]
        pool, remaining = sum([portions[i] for i in candidates]), surplus
        for i in candidates:
            more = min(most - given[i], max(1, remaining * portions[i] // pool), surplus)
            given[i] = given[i] + more
            surplus = surplus - more
    return np.array([most] + given)


def ragged(own_key, count, total, most, lean):
    if count == 2:
        one = jax.random.randint(own_key, (), max(1, total - most), min(most, total - 1) + 1)
        return jnp.stack([one, total - one])
    sizes = jnp.asarray(split_up(count, total, most, lean), jnp.int32)
    couples = (count - 1) // 2
    donor, sink = sizes[1:1 + 2 * couples:2], sizes[2:2 + 2 * couples:2]
    margin = jnp.minimum(donor - 1, most - sink)
    moved = jax.random.randint(jax.random.fold_in(own_key, 1), (couples,), 0, 1 << 20) % (margin + 1)
    sizes = sizes.at[1:1 + 2 * couples:2].set(donor - moved).at[2:2 + 2 * couples:2].set(sink + moved)
    return sizes[jax.random.permutation(jax.random.fold_in(own_key, 2), count)]


def scatter_about(own_key, shape, spread, limit, shards=(), held_as=jnp.bfloat16):
    gain = level_of(own_key, shape, shards, -0.22, 0.18) if shards else 1.0
    drawn = jax.random.normal(own_key, shape, jnp.float32) * spread * gain
    return jnp.minimum(jnp.maximum(drawn, -limit), limit).astype(held_as)


def noise_with(rng, shape, width, reach, split, heavy, kind=jnp.bfloat16):
    values = width * jax.random.normal(rng, shape, jnp.float32)
    if split:
        values = values * level_of(rng, shape, split, -0.22, 0.18)
    return jnp.clip(with_spikes(values, jax.random.fold_in(rng, 3), *heavy), -reach, reach).astype(kind)


def setup_inputs(seed: int = 0) -> dict:
    seeds = jax.random.split(jax.random.key(seed), 8)
    q_latent = draw_q_latent(jax.random.fold_in(seeds[7], 71), 0)
    kv_latent = scatter_about(seeds[1], (TOKENS, KL + ROPE), 1.0, 6.0, ((0, 8),))
    kv_gain = jnp.clip(1.0 + 0.18 * jax.random.normal(seeds[2], (KL,), jnp.float32), 0.1, 1.9)
    q_weight = scatter_about(seeds[3], (QL, HEADS * (NOPE + ROPE)), QL ** -0.5, 0.15625, ((0, 8), (1, 4)))
    kv_weight = scatter_about(seeds[4], (KL, HEADS * (NOPE + VDIM)), KL ** -0.5, 0.25, ((0, 8), (1, 4)))
    out_weight = noise_with(seeds[5], (HEADS * VDIM, D), (HEADS * VDIM) ** -0.5, 0.125, ((0, 4), (1, 8)), (0, 1, 8, 2.0))
    documents = jnp.searchsorted(jnp.cumsum(ragged(seeds[6], N_CTX // 2, TOKENS, 4 * TOK_DEV, 2)), jnp.arange(TOKENS), side="right").astype(jnp.int32)
    return dict(q_latent=q_latent, kv_latent=kv_latent, kv_gain=kv_gain, q_weight=q_weight, kv_weight=kv_weight, out_weight=out_weight, documents=documents)


epsilon = 1e-06

def rotate(inputs, positions):
    half_width = inputs.shape[-1] // 2
    inverse = 10000.0 ** (-2.0 * jnp.arange(half_width, dtype=jnp.float32) / inputs.shape[-1])
    angles = positions.astype(jnp.float32)[:, None] * inverse[None, :]
    shape = (angles.shape[0],) + (1,) * (inputs.ndim - 2) + (half_width,)
    cosine = jnp.cos(angles).reshape(shape)
    sine_part = jnp.sin(angles).reshape(shape)
    front_half = inputs[..., :half_width]
    back_half = inputs[..., half_width:]
    return jnp.concatenate([front_half * cosine - back_half * sine_part, back_half * cosine + front_half * sine_part], axis=-1)

def reference(q_latent, kv_latent, kv_gain, q_weight, kv_weight, out_weight, documents):
    tokens = q_latent.shape[0]
    head_count = HEAD_DEV * N_GRP
    positions = jnp.arange(tokens, dtype=jnp.int32)
    query = jnp.dot(q_latent, q_weight, preferred_element_type=jnp.float32).reshape(tokens, head_count, NOPE + ROPE)
    query_nope = query[..., :NOPE].astype(jnp.bfloat16)
    query_rope = rotate(query[..., NOPE:], positions).astype(jnp.bfloat16)
    latent = kv_latent[:, :KL].astype(jnp.float32)
    normed = latent * lax.rsqrt(lax.optimization_barrier(jnp.mean(latent * latent, axis=-1, keepdims=True)) + epsilon) * kv_gain.astype(jnp.float32)
    normed = normed.astype(jnp.bfloat16)
    key_rope = rotate(kv_latent[:, KL:].astype(jnp.float32), positions).astype(jnp.bfloat16)
    key_value = jnp.dot(normed, kv_weight, preferred_element_type=jnp.float32).astype(jnp.bfloat16)
    key_value = key_value.reshape(tokens, head_count, NOPE + VDIM)
    key_nope = jnp.pad(key_value[..., :NOPE], ((TOK_DEV, 0), (0, 0), (0, 0)))
    values = jnp.pad(key_value[..., NOPE:], ((TOK_DEV, 0), (0, 0), (0, 0)))
    key_rope = jnp.pad(key_rope, ((TOK_DEV, 0), (0, 0)))
    key_docs = jnp.concatenate([jnp.full((TOK_DEV,), -1, jnp.int32), documents.astype(jnp.int32)])
    scale = (NOPE + ROPE) ** (-0.5)

    def one_block(block_index):
        start = (block_index * TOK_DEV).astype(jnp.int32)
        q_nope = lax.dynamic_slice_in_dim(query_nope, start, TOK_DEV, 0).astype(jnp.float32)
        q_rope = lax.dynamic_slice_in_dim(query_rope, start, TOK_DEV, 0).astype(jnp.float32)
        k_nope = lax.dynamic_slice_in_dim(key_nope, start, 2 * TOK_DEV, 0).astype(jnp.float32)
        k_rope = lax.dynamic_slice_in_dim(key_rope, start, 2 * TOK_DEV, 0).astype(jnp.float32)
        v_block = lax.dynamic_slice_in_dim(values, start, 2 * TOK_DEV, 0).astype(jnp.float32)
        q_docs = lax.dynamic_slice_in_dim(documents.astype(jnp.int32), start, TOK_DEV, 0)
        k_docs = lax.dynamic_slice_in_dim(key_docs, start, 2 * TOK_DEV, 0)
        q_pos = start + jnp.arange(TOK_DEV, dtype=jnp.int32)
        k_pos = start - TOK_DEV + jnp.arange(2 * TOK_DEV, dtype=jnp.int32)
        scores = (jnp.einsum('qhd,khd->hqk', q_nope, k_nope) + jnp.einsum('qhr,kr->hqk', q_rope, k_rope)) * scale
        allowed = (k_docs[None, :] == q_docs[:, None]) & (k_pos[None, :] <= q_pos[:, None])
        scores = jnp.where(allowed[None], scores, -1e+30)
        highest = lax.optimization_barrier(jnp.max(scores, axis=-1, keepdims=True))
        weights = jnp.exp(scores - highest)
        probs = (weights / lax.optimization_barrier(jnp.sum(weights, axis=-1, keepdims=True))).astype(jnp.bfloat16)
        attended = jnp.einsum('hqk,khv->qhv', probs.astype(jnp.float32), v_block).astype(jnp.bfloat16)
        return attended.reshape(TOK_DEV, head_count * VDIM)
    attended = lax.map(one_block, jnp.arange(N_CTX, dtype=jnp.int32)).reshape(tokens, N_GRP, HEAD_DEV * VDIM)
    weight_groups = out_weight.reshape(N_GRP, HEAD_DEV * VDIM, D)

    def add_group(running, group):
        rows = lax.dynamic_index_in_dim(attended, group, 1, keepdims=False)
        matrix = lax.dynamic_index_in_dim(weight_groups, group, 0, keepdims=False)
        partial_value = jnp.dot(rows, matrix, preferred_element_type=jnp.float32).astype(jnp.bfloat16)
        partial_value = lax.optimization_barrier(partial_value)
        return (running + partial_value.astype(jnp.float32), None)
    mixed, unused = lax.scan(add_group, jnp.zeros((tokens, D), jnp.float32), jnp.arange(N_GRP, dtype=jnp.int32))
    return mixed.astype(jnp.bfloat16)
```

```python
import jax
import jax.numpy as jnp
from jax import lax
from jax.sharding import PartitionSpec as P

KL = 512
NOPE = 128
ROPE = 64
VDIM = 128


epsilon = 1e-06


def shifted(block, axis, distance):
    devices = range(lax.axis_size(axis))
    route = [(i - distance, i) for i in devices if i - distance in devices]
    return lax.ppermute(block, axis, route)


def rotate(inputs, positions):
    half_width = inputs.shape[-1] // 2
    inverse = 10000.0 ** (-2.0 * jnp.arange(half_width, dtype=jnp.float32) / inputs.shape[-1])
    angles = positions.astype(jnp.float32)[:, None] * inverse[None, :]
    shape = (angles.shape[0],) + (1,) * (inputs.ndim - 2) + (half_width,)
    cosine = jnp.cos(angles).reshape(shape)
    sine_part = jnp.sin(angles).reshape(shape)
    front_half = inputs[..., :half_width]
    back_half = inputs[..., half_width:]
    return jnp.concatenate(
        [front_half * cosine - back_half * sine_part, back_half * cosine + front_half * sine_part],
        axis=-1,
    )


def prepare(latent_block, positions, kv_gain):
    latent = latent_block[:, :KL].astype(jnp.float32)
    normed = (
        latent * lax.rsqrt(jnp.mean(latent * latent, axis=-1, keepdims=True) + epsilon) * kv_gain
    )
    key_rope = rotate(latent_block[:, KL:].astype(jnp.float32), positions).astype(jnp.bfloat16)
    return (normed.astype(jnp.bfloat16), key_rope)


def folder(left, weight_piece):
    return jnp.dot(left, weight_piece, preferred_element_type=jnp.float32)


def per_device(q_latent, kv_latent, kv_gain, q_weight, kv_weight, out_weight, documents):
    rows_dev = q_latent.shape[0]
    head_count = q_weight.shape[1] // (NOPE + ROPE)
    block_index = lax.axis_index("ctx")
    query_pos = block_index * rows_dev + jnp.arange(rows_dev, dtype=jnp.int32)
    prior_pos = query_pos - rows_dev
    query_full = folder(q_latent, lax.all_gather(q_weight, "ctx", axis=0, tiled=True))
    query_full = query_full.reshape(rows_dev, head_count, NOPE + ROPE)
    query_nope = query_full[..., :NOPE].astype(jnp.bfloat16)
    query_rope = rotate(query_full[..., NOPE:], query_pos).astype(jnp.bfloat16)
    previous = shifted(kv_latent, "ctx", 1)
    latent_block = jnp.concatenate([previous, kv_latent], axis=0)
    positions = jnp.concatenate([prior_pos, query_pos])
    normed, key_rope = prepare(latent_block, positions, kv_gain)
    key_value = folder(normed, lax.all_gather(kv_weight, "ctx", axis=0, tiled=True))
    key_value = key_value.astype(jnp.bfloat16)
    key_value = key_value.reshape(2 * rows_dev, head_count, NOPE + VDIM)
    key_nope = key_value[..., :NOPE]
    values = key_value[..., NOPE:]
    key_pos = jnp.concatenate([prior_pos, query_pos])
    query_docs = lax.dynamic_slice_in_dim(documents, block_index * rows_dev, rows_dev, 0)
    prior_docs = lax.dynamic_slice_in_dim(
        documents, jnp.maximum(block_index - 1, 0) * rows_dev, rows_dev, 0
    )
    key_docs = jnp.concatenate([prior_docs, query_docs])
    allowed = (
        (key_docs[None, :] == query_docs[:, None])
        & (key_pos[None, :] <= query_pos[:, None])
        & (key_pos[None, :] >= 0)
    )
    scale = (NOPE + ROPE) ** (-0.5)
    scores = jnp.einsum("qhd,khd->hqk", query_nope, key_nope, preferred_element_type=jnp.float32)
    scores = (
        scores + jnp.einsum("qhr,kr->hqk", query_rope, key_rope, preferred_element_type=jnp.float32)
    ) * scale
    scores = jnp.where(allowed[None], scores, -1e30)
    highest = jnp.max(scores, axis=-1, keepdims=True)
    weights = jnp.exp(scores - highest)
    probs = (weights / jnp.sum(weights, axis=-1, keepdims=True)).astype(jnp.bfloat16)
    attended = jnp.einsum("hqk,khv->qhv", probs, values, preferred_element_type=jnp.float32).astype(
        jnp.bfloat16
    )
    attended = attended.reshape(rows_dev, head_count * VDIM)
    partial_value = jnp.dot(
        attended,
        lax.all_gather(out_weight, "ctx", axis=1, tiled=True),
        preferred_element_type=jnp.float32,
    )
    mixed = lax.psum_scatter(
        partial_value.astype(jnp.bfloat16), "grp", scatter_dimension=1, tiled=True
    )
    return mixed


def flip_route(**bits):
    mask = sum(bits.get(name, 0) << place for place, name in enumerate(("c", "x", "y", "zl", "zh")))
    return [(i, i ^ mask) for i in range(32)]


BOTH = ("ctx", "grp")


def flip(block, **bits):
    return lax.ppermute(block, BOTH, flip_route(**bits))


def route(block, rule):
    pairs = []
    for i in range(32):
        zh, zl, y, x, c = [(i >> place) & 1 for place in (4, 3, 2, 1, 0)]
        there = rule(zh, zl, y, x, c)
        if there is not None:
            zh, zl, y, x, c = there
            pairs.append((i, 16 * zh + 8 * zl + 4 * y + 2 * x + c))
    return lax.ppermute(block, BOTH, pairs)


def ordered(bit, mine, other, axis):
    return jnp.where(
        bit == 0,
        jnp.concatenate([mine, other], axis=axis),
        jnp.concatenate([other, mine], axis=axis),
    )


def halved(weight, bit):
    width = weight.shape[1] // 2
    return lax.dynamic_slice_in_dim(weight, bit * width, width, 1)


def gathered(mine, near, far, across, bits):
    zh, zl, y = bits
    rows = mine.shape[0]
    blocks = {(0, 0): mine, (0, 1): near, (1, 0): far, (1, 1): across}
    whole = jnp.zeros((8 * rows, mine.shape[1]), mine.dtype)
    first = flip(jnp.concatenate([mine, near], axis=0), y=1)
    twins = {
        (0, 0): first[:rows],
        (0, 1): first[rows:],
        (1, 0): flip(far, y=1),
        (1, 1): flip(across, y=1),
    }
    for side, group in ((0, blocks), (1, twins)):
        for (a, b), block in group.items():
            place = 4 * (zh ^ a) + 2 * (zl ^ b) + (y ^ side)
            whole = lax.dynamic_update_slice_in_dim(whole, block, place * rows, 0)
    return whole


def halves(q_latent, kv_latent, kv_gain, q_weight, kv_weight, out_weight, documents):
    rows = q_latent.shape[0]
    width = q_latent.shape[1]
    heads = q_weight.shape[1] // (NOPE + ROPE) // 2
    ctx, grp = lax.axis_index("ctx"), lax.axis_index("grp")
    zh, zl, y, x, c = ctx // 4, ctx // 2 % 2, ctx % 2, grp // 2, grp % 2

    latents = jnp.concatenate([q_latent, kv_latent], axis=1)
    latents = lax.dynamic_slice_in_dim(latents, c * (rows // 2), rows // 2, 0)
    near = flip(latents, zl=1)
    pair = ordered(zl, latents[None], near[None], 0)
    kv_pair = pair[:, :, width:]
    kv_twin = flip(kv_pair, y=1)
    before = route(
        kv_pair[1], lambda zh, zl, y, x, c: (1, zl, 0, x, c) if zh == 0 and y == 1 else None
    )
    extra = jnp.concatenate([kv_twin, before[None]], axis=0)
    pair = ordered(c, pair, flip(pair, c=1), 1)
    extra = ordered(c, extra, flip(extra, c=1), 1)
    query_in = pair[:, :, :width].reshape(2 * rows, width)
    own = pair[:, :, width:]
    prior0 = jnp.where(y == 0, extra[2], extra[0])
    prior1 = jnp.where(y == 0, extra[0], extra[1])
    key_in = jnp.concatenate([prior0, own[0], prior1, own[1]], axis=0)

    q_mine, q_other = halved(q_weight, zl), halved(q_weight, 1 - zl)
    kv_mine, kv_other = halved(kv_weight, zl), halved(kv_weight, 1 - zl)
    kv_full = gathered(
        kv_mine,
        flip(kv_other, zl=1),
        flip(kv_mine, zh=1),
        flip(kv_other, zh=1, zl=1),
        (zh, zl, y),
    )
    q_full = gathered(
        q_mine, flip(q_other, zl=1), flip(q_mine, zh=1), flip(q_other, zh=1, zl=1), (zh, zl, y)
    )

    blocks = 4 * zh + 2 * jnp.arange(2, dtype=jnp.int32) + y
    offsets = jnp.arange(rows, dtype=jnp.int32)
    query_pos = blocks[:, None] * rows + offsets[None, :]
    key_pos = jnp.concatenate([query_pos - rows, query_pos], axis=1)
    normed, key_rope = prepare(key_in, key_pos.reshape(-1), kv_gain)
    key_value = folder(normed, kv_full).astype(jnp.bfloat16)
    key_value = key_value.reshape(2, 2 * rows, heads, NOPE + VDIM)
    key_rope = key_rope.reshape(2, 2 * rows, ROPE)
    query = folder(query_in, q_full).reshape(2 * rows, heads, NOPE + ROPE)
    query_nope = query[..., :NOPE].astype(jnp.bfloat16).reshape(2, rows, heads, NOPE)
    query_rope = rotate(query[..., NOPE:], query_pos.reshape(-1)).astype(jnp.bfloat16)
    query_rope = query_rope.reshape(2, rows, heads, ROPE)
    query_docs = documents[query_pos]
    key_docs = documents[jnp.maximum(key_pos, 0)]
    allowed = (
        (key_docs[:, None, :] == query_docs[:, :, None])
        & (key_pos[:, None, :] <= query_pos[:, :, None])
        & (key_pos[:, None, :] >= 0)
    )
    scale = (NOPE + ROPE) ** (-0.5)
    scores = jnp.einsum(
        "bqhd,bkhd->bhqk", query_nope, key_value[..., :NOPE], preferred_element_type=jnp.float32
    )
    scores = (
        scores
        + jnp.einsum("bqhr,bkr->bhqk", query_rope, key_rope, preferred_element_type=jnp.float32)
    ) * scale
    scores = jnp.where(allowed[:, None], scores, -1e30)
    highest = jnp.max(scores, axis=-1, keepdims=True)
    weights = jnp.exp(scores - highest)
    probs = (weights / jnp.sum(weights, axis=-1, keepdims=True)).astype(jnp.bfloat16)
    attended = jnp.einsum(
        "bhqk,bkhv->bqhv", probs, key_value[..., NOPE:], preferred_element_type=jnp.float32
    ).astype(jnp.bfloat16)
    attended = attended.reshape(2 * rows, heads * VDIM)

    near = flip(attended, zl=1)
    mine = ordered(zl, attended, near, 1)
    twin = ordered(zl, flip(attended, y=1), flip(near, y=1), 1)
    columns = out_weight.shape[1]
    cuts = [(0, columns // 256 * 128), (columns // 256 * 128, columns)]
    pieces = []
    for tokens in (mine, twin):
        tokens = tokens.reshape(2, rows, -1)
        keep = lax.dynamic_index_in_dim(tokens, c, 0, keepdims=False)
        give = lax.dynamic_index_in_dim(tokens, 1 - c, 0, keepdims=False)
        parts = []
        for begin, end in cuts:
            chunk = out_weight[:, begin:end]
            chunk_far = flip(chunk, zh=1)
            sums = []
            for weight in (chunk, chunk_far):
                got = flip(folder(give, weight).astype(jnp.bfloat16), c=1)
                sums.append(folder(keep, weight) + got.astype(jnp.float32))
            here, there = sums
            got_here = route(
                here.astype(jnp.bfloat16),
                lambda zh, zl, y, x, c: (zh, zl, y, 1 - x, c) if x != zh else None,
            )
            got_there = route(
                there.astype(jnp.bfloat16),
                lambda zh, zl, y, x, c: (zh, zl, y, 1 - x, c) if x == zh else None,
            )
            parts.append(
                jnp.where(
                    x == zh,
                    here + got_here.astype(jnp.float32),
                    there + got_there.astype(jnp.float32),
                ).astype(jnp.bfloat16)
            )
        pieces.append(parts)
    same = [route(p, lambda zh, zl, y, x, c: (zh, c, y, x, zl)) for p in pieces[0]]
    cross = [route(p, lambda zh, zl, y, x, c: (zh, c, 1 - y, x, zl)) for p in pieces[1]]
    return ordered(y, jnp.concatenate(same, axis=1), jnp.concatenate(cross, axis=1), 1)


def solution(mesh):
    placed = (
        P("ctx", None),
        P("ctx", None),
        P(),
        P("ctx", "grp"),
        P("ctx", "grp"),
        P("grp", "ctx"),
        P(),
    )
    body = halves if (mesh.shape["ctx"], mesh.shape["grp"]) == (8, 4) else per_device
    return jax.shard_map(
        body, mesh=mesh, in_specs=placed, out_specs=P("ctx", "grp"), check_vma=False
    )
```
